32 devices in a mesh: gx: 4 (over y, x), gy: 2 (over core), gz: 4 (over z).
Axes of the slice: x: 2, y: 2, z: 4, core: 2. Of those that a mesh axis runs over, the one named last changes fastest.
Arguments:
- params: float32 [12, 7168, 1536], P('gx', 'gy', 'gz'), may hold values from -100 to 100
- grads: bfloat16 [12, 7168, 1536], P('gx', 'gy', 'gz'), may hold values from -300 to 300
- row_state: float32 [12, 7168], P('gx', 'gy'), may hold values from 0.01 to 1
- col_state: float32 [12, 1536], P('gx', 'gz'), may hold values from 0.01 to 1
Outputs:
- new_params: float32 [12, 7168, 1536], P('gx', 'gy', 'gz')
- row_new: float32 [12, 7168], P('gx', 'gy')
- col_new: float32 [12, 1536], P('gx', 'gz')
- applied_step: float32 [12, 7168, 1536], P('gx', 'gy', 'gz')
- compute_copy: bfloat16 [12, 7168, 1536], P('gx', 'gy')
The draws below stay inside these ranges and needn't reach their ends.
All inputs are finite; a program needn't handle non-finite values.
Results may differ from the reference program's by a relative error of at most 0.0004.
Values may be sent and summed in bfloat16 or wider, within the bound.
A program may use at most 192 MiB of HBM per device.

```python
import math
import jax
import jax.numpy as jnp
from jax import lax

D = 7168
QR = 1536
LAY = 12


def draw_params(key, part):
    subkeys = jax.random.split(jax.random.fold_in(key, 17), 3)
    normal_part = jnp.clip(jax.random.normal(subkeys[0], (LAY, D, QR), jnp.float32), -6.0, 6.0)
    row_rise = jnp.arange(D, dtype=jnp.float32) / D
    col_rise = jnp.arange(QR, dtype=jnp.float32) / QR
    row_scale = 10.0 ** (0.5 * row_rise + 0.4 * jax.random.uniform(subkeys[1], (D,), jnp.float32) - 0.45)
    col_scale = 10.0 ** (0.5 * col_rise + 0.4 * jax.random.uniform(subkeys[2], (QR,), jnp.float32) - 0.45)
    weights = normal_part * row_scale[None, :, None] * col_scale[None, None, :]
    return weights.astype(jnp.float32)


def draw_grads(key, part):
    subkeys = jax.random.split(key, 3)
    normal_part = jnp.clip(jax.random.normal(subkeys[0], (LAY, D, QR), jnp.float32), -6.0, 6.0)
    row_rise = jnp.arange(D, dtype=jnp.float32) / D
    col_rise = jnp.arange(QR, dtype=jnp.float32) / QR
    layer_rise = jnp.arange(LAY, dtype=jnp.float32) / LAY
    row_scale = 10.0 ** (0.5 * row_rise + 0.5 * jax.random.uniform(subkeys[1], (D,), jnp.float32) - 0.5)
    col_scale = 10.0 ** (0.5 * col_rise + 0.5 * jax.random.uniform(subkeys[2], (QR,), jnp.float32) - 0.5)
    layer_scale = 10.0 ** (0.25 * layer_rise)
    gradient = normal_part * row_scale[None, :, None] * col_scale[None, None, :] * layer_scale[:, None, None]
    return gradient.astype(jnp.bfloat16)


def steps_of(own_key, dims, shards, least, top_value):
    def one(dim, shards_of):
        draws = jax.random.uniform(jax.random.fold_in(jax.random.fold_in(own_key, 6), dim), (shards_of,), jnp.float32, least / len(shards), top_value / len(shards))
        return jnp.repeat(jnp.exp(draws), dims[dim] // shards_of).reshape((-1,) + (1,) * (len(dims) - dim - 1))

    level = one(*shards[0])
    for cut in shards[1:]:
        level = level * one(*cut)
    return level


def setup_inputs(seed: int = 0) -> dict:
    streams_of = jax.random.split(jax.random.key(seed), 5)
    return {
        "params": draw_params(jax.random.fold_in(streams_of[4], 71), 0),
        "grads": draw_grads(jax.random.fold_in(streams_of[4], 71), 0),
        "row_state": jnp.clip(jnp.exp(math.log(1.0) - 4.6051702 * jax.random.uniform(streams_of[2], (LAY, D), jnp.float32) ** steps_of(streams_of[2], (LAY, D), ((0, 4), (1, 2)), -0.2, 0.2)), 0.01, 1.0),
        "col_state": jnp.clip(jnp.exp(math.log(1.0) - 4.6051702 * jax.random.uniform(streams_of[3], (LAY, QR), jnp.float32) ** steps_of(streams_of[3], (LAY, QR), ((0, 4), (1, 4)), -0.2, 0.2)), 0.01, 1.0),
    }


decay_rate = 0.842
tiny_term = 1e-30
step_share = 0.01
clip_limit = 1.0

def layer_factors(weights, gradient, row_old, col_old):
    grad_float = gradient.astype(jnp.float32)
    squares = grad_float * grad_float + tiny_term
    row_new = decay_rate * row_old + (1.0 - decay_rate) * lax.optimization_barrier(jnp.mean(squares, axis=1))
    col_new = decay_rate * col_old + (1.0 - decay_rate) * lax.optimization_barrier(jnp.mean(squares, axis=0))
    row_norm = row_new / jnp.mean(row_new)
    update = grad_float * lax.rsqrt(row_norm[:, None] * col_new[None, :])
    weight_scale = jnp.sqrt(jnp.mean(weights * weights))
    return (update, weight_scale, row_new, col_new)

def reference(params, grads, row_state, col_state):

    def measure_layer(operands):
        update, weight_scale, row_new, col_new = layer_factors(*operands)
        return (jnp.sum(update * update), weight_scale, row_new, col_new)
    update_sq, weight_scale, row_new, col_new = lax.map(measure_layer, (params, grads, row_state, col_state))
    root_mean = jnp.sqrt(jnp.sum(update_sq) / params.size)
    clip_factor = jnp.maximum(1.0, root_mean / clip_limit)

    def apply_layer(operands):
        weights, gradient, row_old, col_old, layer_scale = operands
        update = layer_factors(weights, gradient, row_old, col_old)[0]
        applied = layer_scale * update / clip_factor
        return (applied, weights - step_share * applied)
    applied_step, new_params = lax.map(apply_layer, (params, grads, row_state, col_state, weight_scale))
    return (new_params, row_new, col_new, applied_step, new_params.astype(jnp.bfloat16))
```

```python
import functools
import jax
import jax.numpy as jnp
from jax import lax
from jax.experimental import pallas as pl
from jax.experimental.pallas import tpu as pltpu
from jax.sharding import PartitionSpec as P

decay_rate = 0.842
tiny_term = 1e-30
step_share = 0.01
clip_limit = 1.0
LANES = 128
f32, bf16 = jnp.float32, jnp.bfloat16


def fold(values):
    return jnp.sum(values.reshape(values.shape[0] // 8, 8, values.shape[1]), axis=0)


def fold_lanes(row):
    return sum(row[:, i : i + LANES] for i in range(0, row.shape[1], LANES))


def split(values):
    high = values.astype(bf16)
    return high, (values - high.astype(f32)).astype(bf16)


def row_dots(left, values):
    dims = (((1,), (1,)), ((), ()))
    high, low = split(values)
    return lax.dot_general(left, high, dims, preferred_element_type=f32) + lax.dot_general(
        left, low, dims, preferred_element_type=f32
    )


def exchange(axis, bufs, send, recv):
    n, me = lax.axis_size(axis), lax.axis_index(axis)
    copies = []
    for i, buf in enumerate(bufs):
        for d in range(1, n):
            slot = i * (n - 1) + d - 1
            copy = pltpu.make_async_remote_copy(
                src_ref=buf.at[me],
                dst_ref=buf.at[me],
                send_sem=send.at[slot],
                recv_sem=recv.at[slot],
                device_id={axis: lax.rem(me + d, n)},
                device_id_type=pl.DeviceIdType.MESH,
            )
            copy.start()
            copies.append(copy)
    return copies


def finish(copies):
    for copy in copies:
        copy.wait()


def total(buf):
    return functools.reduce(lambda a, b: a + b, [buf[i] for i in range(buf.shape[0])])


def stats_kernel(
    layers, chunk, small,
    p_hbm, g_hbm, row_ref, col_ref,
    row_out, col_out, rr_out, rc_out, big_hbm, small_hbm,
    p_vm, g_vm, new_vm, row_all, col_all, sc_z, sc_y, up_z, up_y, up_x,
    p_sem, g_sem, o_sem,
    rz_s, rz_r, cy_s, cy_r, sy_s, sy_r, uz_s, uz_r, uy_s, uy_r, ux_s, ux_r,
):
    rows_total, columns = g_vm.shape
    rows = rows_total // layers
    nb, per, chunks = rows // LANES, chunk // LANES, rows // chunk
    nx, ny, nz = (lax.axis_size(a) for a in ("gx", "gy", "gz"))
    me_x, me_y, me_z = (lax.axis_index(a) for a in ("gx", "gy", "gz"))
    rows_all, columns_all = rows * ny, columns * nz

    loads = []
    for k in range(layers * chunks):
        part = pl.ds(k * chunk, chunk)
        g_copy = pltpu.make_async_copy(g_hbm.at[part], g_vm.at[part], g_sem.at[k])
        p_copy = pltpu.make_async_copy(p_hbm.at[part], p_vm.at[part], p_sem.at[k])
        g_copy.start()
        p_copy.start()
        loads.append((g_copy, p_copy))

    barrier = pltpu.get_barrier_semaphore()
    for axis, n, me in (("gx", nx, me_x), ("gy", ny, me_y), ("gz", nz, me_z)):
        for d in range(1, n):
            pl.semaphore_signal(
                barrier, inc=1, device_id={axis: lax.rem(me + d, n)},
                device_id_type=pl.DeviceIdType.MESH,
            )
    pl.semaphore_wait(barrier, nx + ny + nz - 3)

    ones = jnp.ones((16, columns), bf16)
    sc_z[me_z] = jnp.zeros(sc_z.shape[1:], f32)
    col_all[me_y] = jnp.zeros(col_all.shape[1:], f32)
    for l in range(layers):
        carry = (jnp.zeros((8, columns), f32), jnp.zeros((8, columns), f32))
        for c in range(chunks):
            k = l * chunks + c
            for copy in loads[k]:
                copy.wait()

            def measure(b, carry, k=k):
                col_sum, weight_sum = carry
                block = k * per + b
                here = pl.ds(pl.multiple_of(block * LANES, LANES), LANES)
                grad = g_vm[here, :].astype(f32)
                squares = grad * grad + tiny_term
                row_all[me_z, pl.ds(block, 1), :] = row_dots(ones, squares)[0:1]
                weights = p_vm[here, :]
                return col_sum + fold(squares), weight_sum + fold(weights * weights)

            carry = lax.fori_loop(0, per, measure, carry, unroll=True)
        col_all[me_y, l : l + 1, :] = jnp.sum(carry[0], axis=0, keepdims=True)
        sc_z[me_z, l : l + 1, :] = fold_lanes(jnp.sum(carry[1], axis=0, keepdims=True))
        own = slice(l * nb, (l + 1) * nb)
        row_part = (decay_rate / nz) * row_ref[own, :] + (
            (1.0 - decay_rate) / columns_all
        ) * row_all[me_z, own, :]
        sc_z[me_z, layers + l : layers + l + 1, :] = jnp.sum(row_part, axis=0, keepdims=True)

    first = exchange("gz", (row_all, sc_z), rz_s, rz_r)
    cols = exchange("gy", (col_all,), cy_s, cy_r)
    finish(first)
    sc_y[me_y] = total(sc_z)
    scalars = exchange("gy", (sc_y,), sy_s, sy_r)
    row_new = decay_rate * row_ref[...] + (1.0 - decay_rate) * (total(row_all) / columns_all)
    row_out[...] = row_new
    finish(cols)
    col_new = decay_rate * col_ref[...] + (1.0 - decay_rate) * (
        total(col_all)[0:layers] / rows_all
    )
    col_out[...] = col_new
    finish(scalars)
    sums = jnp.sum(total(sc_y), axis=1, keepdims=True)
    weight_scale = jnp.sqrt(sums[0:layers] / (rows_all * columns_all))
    row_mean = sums[layers : 2 * layers] / rows_all
    for l in range(layers):
        own = slice(l * nb, (l + 1) * nb)
        rr_out[own, :] = lax.rsqrt(row_out[own, :] / row_mean[l : l + 1])
    col_root = lax.rsqrt(col_new)

    lane_sum = jnp.zeros((1, LANES), f32)
    pick = lax.broadcasted_iota(jnp.int32, (16, columns), 0)
    for l in range(layers):
        inverse = jnp.broadcast_to(col_root[l : l + 1] * col_root[l : l + 1], (16, columns))
        top = inverse.astype(bf16).astype(f32)
        mid = (inverse - top).astype(bf16).astype(f32)
        rest = inverse - top - mid
        left = jnp.where(
            pick == 0, top, jnp.where(pick == 1, mid, jnp.where(pick == 2, rest, 0.0))
        ).astype(bf16)

        def weigh(b, acc, first_block, left=left):
            block = first_block + b
            here = pl.ds(pl.multiple_of(block * LANES, LANES), LANES)
            grad = g_vm[here, :].astype(f32)
            sums = jnp.sum(row_dots(left, grad * grad)[0:8], axis=0, keepdims=True)
            root = rr_out[pl.ds(block, 1), :]
            return acc + sums * (root * root)

        def weigh_chunk(c, acc, l=l, weigh=weigh):
            one = functools.partial(weigh, first_block=l * nb + c * per)
            return lax.fori_loop(0, per, one, acc, unroll=True)

        lane_sum = lax.fori_loop(0, chunks, weigh_chunk, lane_sum)

    up_z[me_z] = jnp.broadcast_to(lane_sum, up_z.shape[1:])
    finish(exchange("gz", (up_z,), uz_s, uz_r))
    up_y[me_y] = total(up_z)
    finish(exchange("gy", (up_y,), uy_s, uy_r))
    up_x[me_x] = total(up_y)
    finish(exchange("gx", (up_x,), ux_s, ux_r))
    update_total = jnp.sum(total(up_x)[0:1], axis=1, keepdims=True)
    entries = layers * nx * rows_all * columns_all
    clip_factor = jnp.maximum(1.0, jnp.sqrt(update_total / entries) / clip_limit)
    col_step = col_root * (weight_scale / clip_factor)
    rc_out[...] = col_step

    stores = []
    for l in range(layers):
        for c in range(chunks):
            k = l * chunks + c

            def apply(b, carry, k=k, l=l):
                block = k * per + b
                here = pl.ds(pl.multiple_of(block * LANES, LANES), LANES)
                root = jnp.broadcast_to(rr_out[pl.ds(block, 1), :], (LANES, LANES)).T
                for j in range(0, columns, LANES):
                    cut = slice(j, j + LANES)
                    applied = g_vm[here, cut].astype(f32) * root * col_step[l : l + 1, cut]
                    new_vm[here, cut] = (p_vm[here, cut] - step_share * applied).astype(bf16)
                return carry

            lax.fori_loop(0, per, apply, 0, unroll=True)
            last = k == layers * chunks - 1
            size = chunk - small if last else chunk
            part = pl.ds(k * chunk, size)
            stores.append(pltpu.make_async_copy(new_vm.at[part], big_hbm.at[part], o_sem.at[k]))
            stores[-1].start()
            if last:
                stores.append(
                    pltpu.make_async_copy(
                        new_vm.at[pl.ds(k * chunk + size, small)], small_hbm, o_sem.at[k + 1]
                    )
                )
                stores[-1].start()
    finish(stores)


def statistics(params, grads, row_state, col_state):
    layers, rows, columns = params.shape
    nx, ny, nz = (lax.axis_size(a) for a in ("gx", "gy", "gz"))
    flat = layers * rows
    nb = rows // LANES
    per = max(q for q in range(1, 9) if nb % q == 0)
    chunk = per * LANES
    small = chunk // 2
    count = layers * (rows // chunk)
    tall = -(-2 * layers // 8) * 8
    sem = lambda n: pltpu.SemaphoreType.DMA((max(n, 1),))
    vmem, anywhere = pl.BlockSpec(memory_space=pltpu.VMEM), pl.BlockSpec(memory_space=pl.ANY)
    blocks = flat // LANES
    pairs = [2 * (nz - 1), ny - 1, ny - 1, nz - 1, ny - 1, nx - 1]
    return pl.pallas_call(
        functools.partial(stats_kernel, layers, chunk, small),
        out_shape=(
            jax.ShapeDtypeStruct((blocks, LANES), f32),
            jax.ShapeDtypeStruct((layers, columns), f32),
            jax.ShapeDtypeStruct((blocks, LANES), f32),
            jax.ShapeDtypeStruct((layers, columns), f32),
            jax.ShapeDtypeStruct((flat - small, columns), bf16),
            jax.ShapeDtypeStruct((small, columns), bf16),
        ),
        in_specs=[anywhere, anywhere, vmem, vmem],
        out_specs=(vmem, vmem, vmem, vmem, anywhere, anywhere),
        scratch_shapes=[
            pltpu.VMEM((flat, columns), f32),
            pltpu.VMEM((flat, columns), bf16),
            pltpu.VMEM((flat, columns), bf16),
            pltpu.VMEM((nz, blocks, LANES), f32),
            pltpu.VMEM((ny, -(-layers // 8) * 8, columns), f32),
            pltpu.VMEM((nz, tall, LANES), f32),
            pltpu.VMEM((ny, tall, LANES), f32),
            pltpu.VMEM((nz, 8, LANES), f32),
            pltpu.VMEM((ny, 8, LANES), f32),
            pltpu.VMEM((nx, 8, LANES), f32),
            sem(count),
            sem(count),
            sem(count + 1),
        ]
        + [sem(n) for n in pairs for _ in range(2)],
        compiler_params=pltpu.CompilerParams(
            collective_id=0, has_side_effects=True, vmem_limit_bytes=60 * 1024 * 1024
        ),
        cost_estimate=pl.CostEstimate(
            flops=20 * flat * columns, bytes_accessed=8 * flat * columns, transcendentals=0
        ),
    )(
        params.reshape(flat, columns),
        grads.reshape(flat, columns),
        row_state.reshape(blocks, LANES),
        col_state,
    )


def place_kernel(n, *refs):
    out = refs[-1]
    columns = out.shape[1] // n
    for d in range(n):
        out[:, d * columns : (d + 1) * columns] = refs[d][0]


def place(gathered, held, row0, flat, block):
    n, rows, columns = gathered.shape
    start = row0 // block
    specs = [pl.BlockSpec((1, block, columns), lambda i, d=d: (d, i, 0)) for d in range(n)]
    operands, aliases = [gathered] * n, {}
    if held is not None:
        operands.append(held)
        specs.append(pl.BlockSpec(memory_space=pl.ANY))
        aliases = {n: 0}
    return pl.pallas_call(
        functools.partial(place_kernel, n),
        grid=(rows // block,),
        in_specs=specs,
        out_specs=pl.BlockSpec((block, n * columns), lambda i: (start + i, 0)),
        out_shape=jax.ShapeDtypeStruct((flat, n * columns), bf16),
        input_output_aliases=aliases,
        cost_estimate=pl.CostEstimate(
            flops=0, bytes_accessed=4 * n * rows * columns, transcendentals=0
        ),
    )(*operands)


def body(params, grads, row_state, col_state):
    layers, rows, columns = params.shape
    row_new, col_new, row_root, col_step, big, small = statistics(
        params, grads, row_state, col_state
    )
    big_all = lax.all_gather(big, "gz", axis=0)
    small_all = lax.all_gather(small, "gz", axis=0)
    row_root = row_root.reshape(layers, rows)
    applied = grads.astype(f32) * row_root[:, :, None] * col_step[:, None, :]
    new_params = params - step_share * applied
    flat, block = layers * rows, small.shape[0]
    held = place(big_all, None, 0, flat, block)
    held = place(small_all, held, big.shape[0], flat, block)
    compute = held.reshape(layers, rows, held.shape[1])
    return (new_params, row_new.reshape(layers, rows), col_new, applied, compute)


def solution(mesh):
    in_specs = (P("gx", "gy", "gz"), P("gx", "gy", "gz"), P("gx", "gy"), P("gx", "gz"))
    out_specs = (
        P("gx", "gy", "gz"),
        P("gx", "gy"),
        P("gx", "gz"),
        P("gx", "gy", "gz"),
        P("gx", "gy", None),
    )
    return jax.shard_map(body, mesh=mesh, in_specs=in_specs, out_specs=out_specs, check_vma=False)
```
